32 devices in a mesh: occ: 8 (over z, y), aux: 4 (over x, core).
Axes of the slice: x: 2, y: 2, z: 4, core: 2. Of those that a mesh axis runs over, the one named last changes fastest.
Arguments:
- amplitudes: bfloat16 [2, 512, 2048], P(None, 'occ'), may hold values from -0.29882812 to 0.29882812
- fit_factor: bfloat16 [1024, 512, 2048], P('aux', 'occ'), may hold values from -0.14941406 to 0.14941406
Outputs:
- virtual_density: float32 [2, 2048, 2048], P(None, 'aux', 'occ')
- occupied_density: float32 [2, 512, 512], P(None, 'occ')
- right_side: float32 [2, 512, 2048], P(None, 'occ', 'aux')
The draws below stay inside these ranges and needn't reach their ends.
All inputs are finite; a program needn't handle non-finite values.
Results may differ from the reference program's by a relative error of at most 0.0068.
Values may be sent and summed in bfloat16 or wider, within the bound.
A program may use at most 128 MiB of HBM per device.

```python
import jax
import jax.numpy as jnp
from jax import lax

OCC = 512
VIRT = 2048
AUXF = 1024
STATES = 2


def block_levels(rng, shape, split, least, high):
    def one(dim, parts):
        heights = jax.random.uniform(jax.random.fold_in(jax.random.fold_in(rng, 6), dim), (parts,), jnp.float32, least / len(split), high / len(split))
        return jnp.repeat(jnp.exp(heights), shape[dim] // parts).reshape((-1,) + (1,) * (len(shape) - dim - 1))

    level = one(*split[0])
    for cut in split[1:]:
        level = level * one(*cut)
    return level


def scatter_about(own_key, extent, scale, limit, cuts=(), dtype=jnp.bfloat16):
    level = block_levels(own_key, extent, cuts, -0.22, 0.18) if cuts else 1.0
    entries = jax.random.normal(own_key, extent, jnp.float32) * scale * level
    return jnp.minimum(jnp.maximum(entries, -limit), limit).astype(dtype)


def setup_inputs(seed: int = 0) -> dict:
    seeds = jax.random.split(jax.random.key(seed), 3)
    amplitudes = scatter_about(seeds[0], (STATES, OCC, VIRT), 0.044, 0.29882812, ((1, 8),))
    fit_factor = scatter_about(seeds[1], (AUXF, OCC, VIRT), 0.023, 0.14941406, ((0, 4), (1, 8)))
    return dict(amplitudes=amplitudes, fit_factor=fit_factor)


def reference(amplitudes, fit_factor):
    wide = amplitudes.astype(jnp.float32)
    high = lax.Precision.HIGHEST
    virtual_density = jnp.einsum("sia,sib->sab", wide, wide, precision=high)
    occupied_density = jnp.einsum("sia,sja->sij", wide, wide, precision=high)
    flat_amp = amplitudes.reshape(STATES, OCC * VIRT)
    flat_fac = fit_factor.reshape(AUXF, OCC * VIRT)
    fitted = jnp.dot(flat_amp, flat_fac.T, preferred_element_type=jnp.float32).astype(jnp.bfloat16)
    field = jnp.dot(fitted, flat_fac, preferred_element_type=jnp.float32).astype(jnp.bfloat16)
    field_wide = field.reshape(STATES, OCC, VIRT).astype(jnp.float32)
    first = jnp.einsum("sib,sab->sia", field_wide, virtual_density, precision=high)
    second = jnp.einsum("sij,sja->sia", occupied_density, field_wide, precision=high)
    return virtual_density, occupied_density, first - second
```

```python
import jax
import jax.numpy as jnp
from jax import lax
from jax.experimental import pallas as pl
from jax.experimental.pallas import tpu as pltpu
from jax.sharding import PartitionSpec as P

SCATTER = True
NT = (((1,), (1,)), ((), ()))


def block_of(total, want):
    while total % want:
        want //= 2
    return want


def fit_kernel(x_ref, b_ref, out_ref):
    states, occ, virt = x_ref.shape
    count = b_ref.shape[0]
    wide = x_ref[...].reshape(states * occ, virt)
    pairs = lax.dot_general(
        b_ref[...].reshape(count * occ, virt), wide, NT, preferred_element_type=jnp.float32
    ).reshape(count, occ, states * occ)
    row = lax.broadcasted_iota(jnp.int32, pairs.shape, 1)
    col = lax.broadcasted_iota(jnp.int32, pairs.shape, 2)
    out_ref[...] = jnp.sum(jnp.where(col % occ == row, pairs, 0.0), axis=1)


def fit_part(amplitudes, factor):
    states, occ, virt = amplitudes.shape
    aux = factor.shape[0]
    count = block_of(aux, 16)
    sums = pl.pallas_call(
        fit_kernel,
        grid=(aux // count,),
        in_specs=[
            pl.BlockSpec((states, occ, virt), lambda k: (0, 0, 0)),
            pl.BlockSpec((count, occ, virt), lambda k: (k, 0, 0)),
        ],
        out_specs=pl.BlockSpec((count, states * occ), lambda k: (k, 0)),
        out_shape=jax.ShapeDtypeStruct((aux, states * occ), jnp.float32),
        compiler_params=pltpu.CompilerParams(vmem_limit_bytes=48 << 20),
        cost_estimate=pl.CostEstimate(
            flops=2 * states * aux * occ * occ * virt,
            bytes_accessed=2 * aux * occ * virt,
            transcendentals=0,
        ),
    )(amplitudes, factor)
    return jnp.sum(sums.reshape(aux, states, occ), axis=2).T


def field_kernel(f_ref, b_ref, out_ref):
    count, occ, virt = b_ref.shape
    states, depth = f_ref.shape
    spread = f_ref[...].astype(jnp.float32)
    row = lax.broadcasted_iota(jnp.int32, (occ, depth), 0)
    col = lax.broadcasted_iota(jnp.int32, (occ, depth), 1)
    keep = col % occ == row
    left = jnp.concatenate(
        [
            jnp.where(keep, jnp.broadcast_to(spread[s : s + 1], (occ, depth)), 0.0)
            for s in range(states)
        ],
        axis=0,
    ).astype(jnp.bfloat16)
    term = jnp.dot(
        left, b_ref[...].reshape(depth, virt), preferred_element_type=jnp.float32
    ).reshape(states, occ, virt)

    @pl.when(pl.program_id(0) == 0)
    def _():
        out_ref[...] = term

    @pl.when(pl.program_id(0) > 0)
    def _():
        out_ref[...] += term


def field_part(fitted, factor):
    states = fitted.shape[0]
    aux, occ, virt = factor.shape
    count = block_of(aux, 16)
    return pl.pallas_call(
        field_kernel,
        grid=(aux // count,),
        in_specs=[
            pl.BlockSpec((states, count * occ), lambda k: (0, k)),
            pl.BlockSpec((count, occ, virt), lambda k: (k, 0, 0)),
        ],
        out_specs=pl.BlockSpec((states, occ, virt), lambda k: (0, 0, 0)),
        out_shape=jax.ShapeDtypeStruct((states, occ, virt), jnp.float32),
        compiler_params=pltpu.CompilerParams(vmem_limit_bytes=48 << 20),
        cost_estimate=pl.CostEstimate(
            flops=2 * states * aux * occ * occ * virt,
            bytes_accessed=2 * aux * occ * virt,
            transcendentals=0,
        ),
    )(jnp.repeat(fitted, occ, axis=1), factor)


def body(amplitudes, fit_factor):
    high = lax.Precision.HIGHEST
    slab = lax.axis_index("aux")
    width = amplitudes.shape[2] // lax.axis_size("aux")
    own_cols = lax.dynamic_slice_in_dim(amplitudes, slab * width, width, 2)
    gathered = lax.all_gather(own_cols, "occ", axis=1, tiled=True)
    blocked = lax.all_to_all(amplitudes, "occ", split_axis=2, concat_axis=1, tiled=True)
    virtual_density = jnp.einsum(
        "sia,sib->sab", gathered, blocked, preferred_element_type=jnp.float32
    )
    pair_part = jnp.einsum("sia,sja->sij", own_cols, gathered, preferred_element_type=jnp.float32)
    occupied_density = lax.psum(pair_part, "aux")
    fitted = lax.psum(fit_part(amplitudes, fit_factor), "occ").astype(jnp.bfloat16)
    part = field_part(fitted, fit_factor)
    if SCATTER:
        field_cols = lax.psum_scatter(part, "aux", scatter_dimension=2, tiled=True).astype(jnp.bfloat16)
    else:
        field = lax.psum(part, "aux").astype(jnp.bfloat16)
        field_cols = lax.dynamic_slice_in_dim(field, slab * width, width, 2)
    second = jnp.einsum(
        "sij,sja->sia",
        occupied_density,
        lax.all_gather(field_cols, "occ", axis=1, tiled=True).astype(jnp.float32),
        precision=high,
    )
    cross_part = jnp.einsum(
        "sib,sjb->sij", field_cols, gathered, preferred_element_type=jnp.float32
    )
    cross = lax.psum(cross_part, "aux")
    first = jnp.einsum("sij,sja->sia", cross, gathered.astype(jnp.float32), precision=high)
    return (virtual_density, occupied_density, first - second)


def solution(mesh):
    placed = (P(None, "occ", None), P("aux", "occ", None))
    return jax.shard_map(
        body,
        mesh=mesh,
        in_specs=placed,
        out_specs=(P(None, "aux", "occ"), P(None, "occ", None), P(None, "occ", "aux")),
        check_vma=False,
    )
```
